32 devices in a mesh: sfc: 32 (over z, y, x, core).
Axes of the slice: x: 2, y: 2, z: 4, core: 2. Of those that a mesh axis runs over, the one named last changes fastest.
Arguments:
- tracers: float32 [2048, 3, 480], P('sfc'), may hold values from -6 to 6
- weights: float32 [2, 2048, 3, 256], P(None, 'sfc'), may hold values from -1.5 to 1.5
- departure: int32 [2048, 48], P('sfc'), may hold values from 0 to 95, as said below
- needs: int32 [32, 8, 4], P('sfc'), may hold values from 0 to 63
- counts: int32 [32, 8], P('sfc'), may hold values from 1 to 4, as said below
Outputs:
- mixed: float32 [2048, 3, 480], P('sfc')
The draws below stay inside these ranges and needn't reach their ends.
Inputs may be any that keep to these rules, and one draw needn't show every extreme that they name: `departure`: each entry is a slot of its range's source table: below 64 a local element; otherwise 64 + j * 4 + c with c below counts[r, j] of its range r. `counts`: some range uses all 4 entries of every list in every draw.
All inputs are finite; a program needn't handle non-finite values.
Results may differ from the reference program's by a relative error of at most 0.0003.
Values sent between devices are 32-bit elements; how exact they have to be, the bound alone decides.
A program may use at most 64 MiB of HBM per device.

```python
import math
import jax
import jax.numpy as jnp
from jax import lax

NODES = 16
TRACERS = 30
LEV = 3
SUBSTEPS = 2
REACH = 4
CAP = 4
ELEMS = 64
ELEMS_ALL = 2048
N_SFC = 32


def counts_table(key):
    ranks_total = ELEMS_ALL // ELEMS
    folded = jax.random.fold_in(key, 11)
    key_counts, key_band = jax.random.split(folded)
    drawn = jax.random.randint(key_counts, (ranks_total, 2 * REACH), 1, CAP + 1)
    band_start = jax.random.randint(key_band, (), 0, ranks_total)
    in_band = (jnp.arange(ranks_total) - band_start) % ranks_total < max(ranks_total // 4, 1)
    return jnp.where(in_band[:, None], CAP, drawn).astype(jnp.int32)


def draw_counts(key, part):
    return counts_table(key)


def draw_departure(key, part):
    limits_table = counts_table(key)
    folded = jax.random.fold_in(key, 23)
    key_remote, key_offset, key_column, key_local = jax.random.split(folded, 4)
    grid_shape = (ELEMS_ALL, LEV * NODES)
    owner_rank = (jnp.arange(ELEMS_ALL) // ELEMS)[:, None]
    remote = jax.random.randint(key_remote, grid_shape, 0, 10) < 3
    offset_pick = jax.random.randint(key_offset, grid_shape, 0, 2 * REACH)
    raw_bits = jax.random.randint(key_column, grid_shape, 0, 1 << 20)
    limits = limits_table[owner_rank, offset_pick]
    column = raw_bits % limits
    local_pick = jax.random.randint(key_local, grid_shape, 0, ELEMS)
    return jnp.where(remote, ELEMS + offset_pick * CAP + column, local_pick).astype(jnp.int32)


def set_ends(entries, rng, smallest, high):
    place = [jax.random.randint(jax.random.fold_in(rng, axis), (), 0, length) for axis, length in enumerate(entries.shape)]
    longest = entries.shape.index(max(entries.shape))
    next_to = place[:longest] + [(place[longest] + 1) % entries.shape[longest]] + place[longest + 1:]
    return entries.at[tuple(place)].set(smallest).at[tuple(next_to)].set(high)


def block_scale(stream_key, extent, cuts, least, top_value):
    gain = 1.0
    for position, shards_of in cuts:
        draws = jax.random.uniform(jax.random.fold_in(jax.random.fold_in(stream_key, 6), position), (shards_of,), jnp.float32, least / len(cuts), top_value / len(cuts))
        gain = gain * jnp.repeat(jnp.exp(draws), extent[position] // shards_of).reshape((-1,) + (1,) * (len(extent) - 1 - position))
    return gain


def normal_values(key, dims, spread, bound, pieces=(), held_as=jnp.bfloat16):
    values = spread * jax.random.normal(key, dims, jnp.float32)
    if pieces:
        values = values * block_scale(key, dims, pieces, -0.22, 0.18)
    return jnp.clip(values, -bound, bound).astype(held_as)


def setup_inputs(seed: int = 0) -> dict:
    seeds = jax.random.split(jax.random.key(seed), 6)
    return {
        "tracers": normal_values(seeds[0], (ELEMS_ALL, LEV, NODES * TRACERS), 1.0, 6.0, ((0, 32),), jnp.float32),
        "weights": normal_values(seeds[1], (SUBSTEPS, ELEMS_ALL, LEV, NODES * NODES), NODES ** -0.5, 1.5, ((1, 32),), jnp.float32),
        "departure": draw_departure(jax.random.fold_in(seeds[5], 71), 0),
        "needs": set_ends(jax.random.randint(seeds[3], (N_SFC, 2 * REACH, CAP), 0, ELEMS), jax.random.fold_in(seeds[3], 1), 0, ELEMS - 1).astype(jnp.int32),
        "counts": draw_counts(jax.random.fold_in(seeds[5], 71), 0),
    }


def interpolate(source_table, dep_block, weight_block):
    elements = dep_block.shape[0]
    block_rows = math.gcd(elements, 32)
    flat_rows = source_table.reshape(-1, NODES * TRACERS)
    slot_rows = dep_block.reshape(elements, LEV, NODES) * LEV + jnp.arange(LEV, dtype=jnp.int32)[None, :, None]

    def per_block(inputs):
        row_index, matrices = inputs
        gathered = flat_rows[row_index].reshape(block_rows, LEV, NODES, NODES, TRACERS)
        matrices = matrices.reshape(block_rows, LEV, NODES, NODES)
        values = jnp.einsum("elts,eltsq->eltq", matrices, gathered, precision=lax.Precision.HIGHEST)
        lowest = jnp.min(gathered, axis=3)
        highest = jnp.max(gathered, axis=3)
        return jnp.clip(values, lowest, highest).reshape(block_rows, LEV, NODES * TRACERS)

    result = lax.map(per_block, (slot_rows.reshape(elements // block_rows, block_rows, LEV, NODES),
                                 weight_block.reshape(elements // block_rows, block_rows, LEV, NODES * NODES)))
    return result.reshape(elements, LEV, NODES * TRACERS)


def reference(tracers, weights, departure, needs, counts):
    offset_order = jnp.arange(2 * REACH, dtype=jnp.int32)
    offsets = jnp.where(offset_order < REACH, offset_order - REACH, offset_order - REACH + 1)
    live_slots = jnp.arange(CAP, dtype=jnp.int32)[None, None, :] < counts[:, :, None]
    current = tracers
    for substep in range(SUBSTEPS):
        def per_range(owner_rank):
            own_rows = lax.dynamic_slice_in_dim(current, owner_rank * ELEMS, ELEMS, 0)
            owners = (owner_rank + offsets) % N_SFC
            row_index = (owners[:, None] * ELEMS + needs[owner_rank]).astype(jnp.int32)
            remote = current[row_index]
            remote = jnp.where(live_slots[owner_rank][:, :, None, None], remote, 0.0)
            source_table = jnp.concatenate([own_rows, remote.reshape(2 * REACH * CAP, LEV, NODES * TRACERS)], axis=0)
            dep_block = lax.dynamic_slice_in_dim(departure, owner_rank * ELEMS, ELEMS, 0)
            weight_block = lax.dynamic_slice_in_dim(weights[substep], owner_rank * ELEMS, ELEMS, 0)
            return interpolate(source_table, dep_block, weight_block)

        current = lax.map(per_range, jnp.arange(N_SFC, dtype=jnp.int32)).reshape(ELEMS_ALL, LEV, NODES * TRACERS)
    return current
```

```python
import jax
import jax.numpy as jnp
from jax import lax
from jax.experimental import pallas as pl
from jax.experimental.pallas import tpu as pltpu
from jax.sharding import PartitionSpec as P

NODES = 16
TRACERS = 30
PADDED = 32
LANES = 128
MESH = pl.DeviceIdType.MESH
F32 = jnp.float32


def kernel(
    tracers_far, weights_far, departure_far, needs_far, counts_far, out,
    tracers, weights, departure, wish, counts, asked, live, mats, state, table, turned,
    sent, got, wish_send, wish_got, row_send, row_got, loaded,
):
    count = lax.axis_size("sfc")
    me = lax.axis_index("sfc")
    substeps, levels, elements, _ = weights.shape
    sides, cap = asked.shape[0], asked.shape[1]
    reach = sides // 2
    narrow = NODES * TRACERS
    remote = sides * cap
    half = NODES // 2
    slots = elements + remote

    def offset_of(j):
        return j - reach + jnp.where(j < reach, 0, 1)

    def device(offset):
        return (lax.rem(me + offset + count, count),)

    barrier = pltpu.get_barrier_semaphore()
    for j in range(sides):
        o = j - reach if j < reach else j - reach + 1
        pl.semaphore_signal(barrier, inc=1, device_id=device(o), device_id_type=MESH)

    loads = [
        pltpu.make_async_copy(far, near, loaded.at[i])
        for i, (far, near) in enumerate((
            (needs_far.at[0], wish), (tracers_far, tracers), (departure_far, departure), (weights_far, weights),
            (counts_far, counts),
        ))
    ]
    for load in loads:
        load.start()

    def wish_copy(j):
        return pltpu.make_async_remote_copy(
            src_ref=wish, dst_ref=asked.at[j],
            send_sem=wish_send.at[j], recv_sem=wish_got.at[j],
            device_id=device(offset_of(j)), device_id_type=MESH,
        )

    def row_copy(s, l, j):
        return pltpu.make_async_remote_copy(
            src_ref=sent.at[s, l, j], dst_ref=got.at[s, l, j],
            send_sem=row_send.at[s, l, j], recv_sem=row_got.at[s, l, j],
            device_id=device(-offset_of(j)), device_id_type=MESH,
        )

    loads[0].wait()
    pl.semaphore_wait(barrier, sides)
    for j in range(sides):
        wish_copy(j).start()

    loads[1].wait()
    for l in range(levels):
        state[0, l, 0:elements, 0:narrow] = tracers[l]

    last = me >= count - reach
    for step in range(sides):
        j = jnp.where(last, sides - 1 - step, step)
        wish_copy(j).wait_recv()
        for l in range(levels):
            for c in range(cap):
                sent[0, l, j, c : c + 1, :] = tracers[l, pl.ds(asked[j, c, j], 1), :]
        for l in range(levels):
            row_copy(0, l, j).start()

    loads[4].wait()
    for j in range(sides):
        for c in range(cap):
            at = j * cap + c
            live[at : at + 1, :] = jnp.full((1, narrow), jnp.where(c < counts[0, j], 1, 0), jnp.int32)

    loads[2].wait()
    loads[3].wait()
    for s in range(substeps):
        for l in range(levels):
            matrix = weights[s, l]
            mats[s, l] = jnp.transpose(jnp.concatenate([matrix[:, : half * NODES], matrix[:, half * NODES :]], axis=0))

    upper = me >= count // 2

    def one_level(s, l):
        for j in range(sides):
            row_copy(s, l, j).wait_recv()
        for j in range(sides):
            at = j * cap
            state[s, l, elements + at : elements + at + cap, 0:narrow] = jnp.where(
                live[at : at + cap, :] > 0, got[s, l, j], 0.0
            )
        table[l] = jnp.transpose(state[s, l])

        first = departure[pl.ds(l * NODES, half), :]
        second = departure[pl.ds(l * NODES + half, half), :]
        both = jnp.concatenate([first, second], axis=1)
        for c in range(half):
            source = jnp.broadcast_to(both[c : c + 1, :], (PADDED, LANES))
            value = lowest = highest = None
            for k in range(NODES):
                item = jnp.take_along_axis(
                    table[l, k * TRACERS : k * TRACERS + PADDED, :], source, axis=1, mode="promise_in_bounds"
                )
                term = mats[s, l, c * NODES + k : c * NODES + k + 1, :] * item
                value = term if k == 0 else value + term
                lowest = item if k == 0 else jnp.minimum(lowest, item)
                highest = item if k == 0 else jnp.maximum(highest, item)
            turned[l, c * TRACERS : c * TRACERS + PADDED, :] = jnp.clip(value, lowest, highest)
        result = jnp.transpose(turned[l])
        near, past = result[:elements, : half * TRACERS], result[elements:, : half * TRACERS]
        if s + 1 < substeps:
            state[s + 1, l, 0:elements, 0 : half * TRACERS] = near
            state[s + 1, l, 0:elements, half * TRACERS : narrow] = past
            for j in range(sides):
                for c in range(cap):
                    sent[s + 1, l, j, c : c + 1, :] = state[s + 1, l, pl.ds(asked[j, c, j], 1), 0:narrow]
            for step in range(sides):
                row_copy(s + 1, l, jnp.where(upper, step, sides - 1 - step)).start()
        else:
            out[l, :, 0 : half * TRACERS] = near
            out[l, :, half * TRACERS : narrow] = past

    for s in range(substeps):
        for l in range(levels):
            one_level(s, l)

    for j in range(sides):
        wish_copy(j).wait_send()
    for s in range(substeps):
        for l in range(levels):
            for j in range(sides):
                row_copy(s, l, j).wait_send()


def on_device(tracers, weights, departure, needs, counts):
    substeps, elements, levels, _ = weights.shape
    sides, cap = needs.shape[1:]
    narrow = NODES * TRACERS
    wide = NODES * PADDED
    half = NODES // 2
    far = pl.BlockSpec(memory_space=pl.ANY)
    result = pl.pallas_call(
        kernel,
        out_shape=pltpu.VMEM((levels, elements, narrow), F32),
        in_specs=[far] * 5,
        out_specs=pl.BlockSpec(memory_space=pltpu.VMEM),
        scratch_shapes=[
            pltpu.VMEM((levels, elements, narrow), F32),
            pltpu.VMEM((substeps, levels, elements, NODES * NODES), F32),
            pltpu.VMEM((levels * NODES, elements), jnp.int32),
            pltpu.SMEM((cap, sides), jnp.int32),
            pltpu.SMEM((1, sides), jnp.int32),
            pltpu.SMEM((sides, cap, sides), jnp.int32),
            pltpu.VMEM((sides * cap, narrow), jnp.int32),
            pltpu.VMEM((substeps, levels, half * NODES, 2 * elements), F32),
            pltpu.VMEM((substeps, levels, LANES, wide), F32),
            pltpu.VMEM((levels, wide, LANES), F32),
            pltpu.VMEM((levels, half * PADDED, 2 * elements), F32),
            pltpu.VMEM((substeps, levels, sides, cap, narrow), F32),
            pltpu.VMEM((substeps, levels, sides, cap, narrow), F32),
            pltpu.SemaphoreType.DMA((sides,)),
            pltpu.SemaphoreType.DMA((sides,)),
            pltpu.SemaphoreType.DMA((substeps, levels, sides)),
            pltpu.SemaphoreType.DMA((substeps, levels, sides)),
            pltpu.SemaphoreType.DMA((5,)),
        ],
        compiler_params=pltpu.CompilerParams(collective_id=0, has_side_effects=True, vmem_limit_bytes=60 << 20),
    )(
        jnp.transpose(tracers, (1, 0, 2)),
        jnp.transpose(weights, (0, 2, 1, 3)),
        jnp.transpose(departure),
        jnp.transpose(needs, (0, 2, 1)),
        counts,
    )
    return jnp.transpose(result, (1, 0, 2))


def solution(mesh):
    return jax.shard_map(
        on_device,
        mesh=mesh,
        in_specs=(
            P("sfc", None, None),
            P(None, "sfc", None, None),
            P("sfc", None),
            P("sfc", None, None),
            P("sfc", None),
        ),
        out_specs=P("sfc", None, None),
        check_vma=False,
    )
```

```python
import jax
import jax.numpy as jnp
from jax import lax
from jax.experimental import pallas as pl
from jax.experimental.pallas import tpu as pltpu
from jax.sharding import PartitionSpec as P

NODES = 16
TRACERS = 30
PADDED = 32
LANES = 128
MESH = pl.DeviceIdType.MESH
F32 = jnp.float32
BF16 = jnp.bfloat16
DENSE = 8


def kernel(
    tracers_far, weights_far, departure_far, needs_far, counts_far, out,
    tracers, weights, departure, wish, counts, asked, live, mats, state, table, turned, parts, picks,
    sent, got, wish_send, wish_got, row_send, row_got, loaded,
):
    count = lax.axis_size("sfc")
    me = lax.axis_index("sfc")
    substeps, levels, elements, _ = weights.shape
    sides, cap = asked.shape[0], asked.shape[1]
    reach = sides // 2
    narrow = NODES * TRACERS
    remote = sides * cap
    half = NODES // 2
    slots = elements + remote

    def offset_of(j):
        return j - reach + jnp.where(j < reach, 0, 1)

    def device(offset):
        return (lax.rem(me + offset + count, count),)

    barrier = pltpu.get_barrier_semaphore()
    for j in range(sides):
        o = j - reach if j < reach else j - reach + 1
        pl.semaphore_signal(barrier, inc=1, device_id=device(o), device_id_type=MESH)

    loads = [
        pltpu.make_async_copy(far, near, loaded.at[i])
        for i, (far, near) in enumerate((
            (needs_far.at[0], wish), (tracers_far, tracers), (departure_far, departure), (weights_far, weights),
            (counts_far, counts),
        ))
    ]
    for load in loads:
        load.start()

    def wish_copy(j):
        return pltpu.make_async_remote_copy(
            src_ref=wish, dst_ref=asked.at[j],
            send_sem=wish_send, recv_sem=wish_got.at[j],
            device_id=device(offset_of(j)), device_id_type=MESH,
        )

    def row_copy(s, l, j):
        return pltpu.make_async_remote_copy(
            src_ref=sent.at[s, l, j], dst_ref=got.at[s, l, j],
            send_sem=row_send, recv_sem=row_got.at[s, l],
            device_id=device(-offset_of(j)), device_id_type=MESH,
        )

    loads[0].wait()
    pl.semaphore_wait(barrier, sides)
    for j in range(sides):
        wish_copy(j).start()

    loads[1].wait()
    for l in range(levels):
        state[0, l, 0:elements, 0:narrow] = tracers[l]

    past_low = count - 1 - me

    def arrival(step):
        low = jnp.where(step <= me, step, jnp.where(step <= reach, step + reach - 1, me + step - reach))
        high = jnp.where(step <= reach - 1 + past_low, sides - 1 - step, step - reach - past_low)
        return jnp.where(me < reach, low, jnp.where(past_low < reach, high, step))

    for step in range(sides):
        j = arrival(step)
        wish_copy(j).wait_recv()
        for l in range(levels):
            for c in range(cap):
                sent[0, l, j, c : c + 1, :] = tracers[l, pl.ds(asked[j, c, j], 1), :]
        for l in range(levels):
            row_copy(0, l, j).start()

    def targets(l):
        first = departure[pl.ds(l * NODES, half), :]
        second = departure[pl.ds(l * NODES + half, half), :]
        return jnp.concatenate([first, second], axis=1)

    loads[4].wait()
    for j in range(sides):
        for c in range(cap):
            at = j * cap + c
            live[at : at + 1, :] = jnp.full((1, narrow), jnp.where(c < counts[0, j], 1, 0), jnp.int32)

    loads[2].wait()
    for s in range(substeps):
        for l in range(levels):
            state[s, l, slots:, :] = jnp.zeros((LANES - slots, NODES * PADDED), F32)
    if DENSE:
        slot_ids = lax.broadcasted_iota(jnp.int32, (2 * LANES, 2 * LANES), 0) % LANES
        for l in range(levels):
            both = targets(l)
            for q in range(DENSE // 2):
                target = jnp.concatenate([both[2 * q : 2 * q + 1, :], both[2 * q + 1 : 2 * q + 2, :]], axis=1)
                picks[l, q] = jnp.where(slot_ids == target, 1.0, 0.0).astype(BF16)
    loads[3].wait()
    for s in range(substeps):
        for l in range(levels):
            matrix = weights[s, l]
            mats[s, l] = jnp.transpose(jnp.concatenate([matrix[:, : half * NODES], matrix[:, half * NODES :]], axis=0))

    upper = me >= count // 2


    def reduce(s, l, c, items):
        value = lowest = highest = None
        for k in range(NODES):
            item = items(k)
            term = mats[s, l, c * NODES + k : c * NODES + k + 1, :] * item
            value = term if k == 0 else value + term
            lowest = item if k == 0 else jnp.minimum(lowest, item)
            highest = item if k == 0 else jnp.maximum(highest, item)
        turned[l, c * TRACERS : c * TRACERS + PADDED, :] = jnp.clip(value, lowest, highest)

    def receive(s, l):
        pltpu.make_async_remote_copy(
            src_ref=sent.at[s, l], dst_ref=got.at[s, l], send_sem=row_send, recv_sem=row_got.at[s, l],
            device_id=device(1), device_id_type=MESH,
        ).wait_recv()

    def arrange(s, l):
        for j in range(sides):
            at = j * cap
            state[s, l, elements + at : elements + at + cap, 0:narrow] = jnp.where(
                live[at : at + cap, :] > 0, got[s, l, j], 0.0
            )
        table[l] = jnp.transpose(state[s, l])
        for k in range(NODES if DENSE else 0):
            block = table[l, k * TRACERS : k * TRACERS + PADDED, :]
            high = block.astype(BF16)
            parts[l, k * PADDED : (k + 1) * PADDED, 0:LANES] = high
            parts[l, k * PADDED : (k + 1) * PADDED, LANES:] = (block - high.astype(F32)).astype(BF16)

    def gather(s, l):
        for q in range(DENSE // 2):
            gathered = jnp.dot(parts[l], picks[l, q], preferred_element_type=F32)
            for side in range(2):
                reduce(s, l, 2 * q + side, lambda k: gathered[k * PADDED : (k + 1) * PADDED, side * LANES : (side + 1) * LANES])
        both = targets(l)
        for c in range(DENSE, half):
            source = jnp.broadcast_to(both[c : c + 1, :], (PADDED, LANES))
            reduce(s, l, c, lambda k: jnp.take_along_axis(
                table[l, k * TRACERS : k * TRACERS + PADDED, :], source, axis=1, mode="promise_in_bounds"
            ))

    def finish(s, l):
        result = jnp.transpose(turned[l])
        near, past = result[:elements, : half * TRACERS], result[elements:, : half * TRACERS]
        if s + 1 < substeps:
            state[s + 1, l, 0:elements, 0 : half * TRACERS] = near
            state[s + 1, l, 0:elements, half * TRACERS : narrow] = past
            for j in range(sides):
                for c in range(cap):
                    sent[s + 1, l, j, c : c + 1, :] = state[s + 1, l, pl.ds(asked[j, c, j], 1), 0:narrow]
        else:
            out[l, :, 0 : half * TRACERS] = near
            out[l, :, half * TRACERS : narrow] = past

    def send(s, l):
        if s + 1 < substeps:
            for step in range(sides):
                row_copy(s + 1, l, jnp.where(upper, step, sides - 1 - step)).start()

    for s in range(substeps):
        for l in range(levels):
            receive(s, l)
            arrange(s, l)
            gather(s, l)
            finish(s, l)
            send(s, l)

    pltpu.make_async_remote_copy(
        src_ref=asked, dst_ref=asked, send_sem=wish_send, recv_sem=wish_got.at[0],
        device_id=device(1), device_id_type=MESH,
    ).wait_send()
    pltpu.make_async_remote_copy(
        src_ref=sent, dst_ref=got, send_sem=row_send, recv_sem=row_got.at[0, 0],
        device_id=device(1), device_id_type=MESH,
    ).wait_send()


def on_device(tracers, weights, departure, needs, counts):
    substeps, elements, levels, _ = weights.shape
    sides, cap = needs.shape[1:]
    narrow = NODES * TRACERS
    wide = NODES * PADDED
    half = NODES // 2
    far = pl.BlockSpec(memory_space=pl.ANY)
    result = pl.pallas_call(
        kernel,
        out_shape=pltpu.VMEM((levels, elements, narrow), F32),
        in_specs=[far] * 5,
        out_specs=pl.BlockSpec(memory_space=pltpu.VMEM),
        scratch_shapes=[
            pltpu.VMEM((levels, elements, narrow), F32),
            pltpu.VMEM((substeps, levels, elements, NODES * NODES), F32),
            pltpu.VMEM((levels * NODES, elements), jnp.int32),
            pltpu.SMEM((cap, sides), jnp.int32),
            pltpu.SMEM((1, sides), jnp.int32),
            pltpu.SMEM((sides, cap, sides), jnp.int32),
            pltpu.VMEM((sides * cap, narrow), jnp.int32),
            pltpu.VMEM((substeps, levels, half * NODES, 2 * elements), F32),
            pltpu.VMEM((substeps, levels, LANES, wide), F32),
            pltpu.VMEM((levels, wide, LANES), F32),
            pltpu.VMEM((levels, half * PADDED, 2 * elements), F32),
            pltpu.VMEM((levels, wide, 2 * LANES), BF16),
            pltpu.VMEM((levels, max(DENSE // 2, 1), 2 * LANES, 2 * LANES), BF16),
            pltpu.VMEM((substeps, levels, sides, cap, narrow), F32),
            pltpu.VMEM((substeps, levels, sides, cap, narrow), F32),
            pltpu.SemaphoreType.DMA,
            pltpu.SemaphoreType.DMA((sides,)),
            pltpu.SemaphoreType.DMA,
            pltpu.SemaphoreType.DMA((substeps, levels)),
            pltpu.SemaphoreType.DMA((5,)),
        ],
        compiler_params=pltpu.CompilerParams(collective_id=0, has_side_effects=True, vmem_limit_bytes=60 << 20),
    )(
        jnp.transpose(tracers, (1, 0, 2)),
        jnp.transpose(weights, (0, 2, 1, 3)),
        jnp.transpose(departure),
        jnp.transpose(needs, (0, 2, 1)),
        counts,
    )
    return jnp.transpose(result, (1, 0, 2))


def solution(mesh):
    return jax.shard_map(
        on_device,
        mesh=mesh,
        in_specs=(
            P("sfc", None, None),
            P(None, "sfc", None, None),
            P("sfc", None),
            P("sfc", None, None),
            P("sfc", None),
        ),
        out_specs=P("sfc", None, None),
        check_vma=False,
    )
```

```python
import jax
import jax.numpy as jnp
from jax import lax
from jax.experimental import pallas as pl
from jax.experimental.pallas import tpu as pltpu
from jax.sharding import PartitionSpec as P

NODES = 16
TRACERS = 30
PADDED = 32
LANES = 128
MESH = pl.DeviceIdType.MESH
F32 = jnp.float32
BF16 = jnp.bfloat16


def kernel(
    tracers_far, weights_far, departure_far, needs_far, counts_far, out,
    tracers, weights, departure, wish, counts, asked, slot_ids, mats, state, table, turned, turned_past, parts, picks,
    sent_first, got_first, sent, got, wish_send, wish_got, row_send, row_got, loaded,
):
    count = lax.axis_size("sfc")
    me = lax.axis_index("sfc")
    substeps, levels, elements, _ = weights.shape
    sides, cap = asked.shape[0], asked.shape[1]
    reach = sides // 2
    narrow = NODES * TRACERS
    remote = sides * cap
    half = NODES // 2
    slots = elements + remote

    def offset_of(j):
        return j - reach + jnp.where(j < reach, 0, 1)

    def device(offset):
        return (lax.rem(me + offset + count, count),)

    loads = [
        pltpu.make_async_copy(far, near, loaded.at[i])
        for i, (far, near) in enumerate((
            (needs_far.at[0], wish), (tracers_far, tracers), (departure_far, departure), (weights_far, weights),
            (counts_far, counts),
        ))
    ]
    loads[0].start()

    barrier = pltpu.get_barrier_semaphore()
    for j in range(sides):
        o = j - reach if j < reach else j - reach + 1
        pl.semaphore_signal(barrier, inc=1, device_id=device(o), device_id_type=MESH)

    for load in loads[1:]:
        load.start()

    def wish_copy(j):
        return pltpu.make_async_remote_copy(
            src_ref=wish, dst_ref=asked.at[j],
            send_sem=wish_send, recv_sem=wish_got.at[j],
            device_id=device(offset_of(j)), device_id_type=MESH,
        )

    def ends(s):
        return (sent_first, got_first) if s == 0 else (sent.at[s - 1], got.at[s - 1])

    def row_copy(s, l, j):
        source, target = ends(s)
        return pltpu.make_async_remote_copy(
            src_ref=source.at[l, j], dst_ref=target.at[l, j], send_sem=row_send.at[s], recv_sem=row_got.at[s, l],
            device_id=device(-offset_of(j)), device_id_type=MESH,
        )

    def rows_of(s, l):
        source, target = ends(s)
        return pltpu.make_async_remote_copy(
            src_ref=source.at[l], dst_ref=target.at[l], send_sem=row_send.at[s], recv_sem=row_got.at[s, l],
            device_id=device(1), device_id_type=MESH,
        )

    loads[0].wait()
    pl.semaphore_wait(barrier, sides)
    upper = me >= count // 2
    for step in range(sides):
        wish_copy(jnp.where(upper, sides - 1 - step, step)).start()

    loads[1].wait()
    for l in range(levels):
        state[0, l, 0:elements, 0:narrow] = tracers[l]

    past_low = count - 1 - me

    def arrival(step):
        low = jnp.where(step <= me, step, jnp.where(step <= reach, step + reach - 1, me + step - reach))
        high = jnp.where(step <= reach - 1 + past_low, sides - 1 - step, step - reach - past_low)
        return jnp.where(me < reach, low, jnp.where(past_low < reach, high, step))

    for step in range(sides):
        j = arrival(step)
        wish_copy(j).wait_recv()
        for l in range(levels):
            for c in range(cap):
                sent_first[l, j, c : c + 1, :] = tracers[l, pl.ds(asked[j, c, j], 1), :]
        for l in range(levels):
            row_copy(0, l, j).start()

    def targets(l):
        first = departure[pl.ds(l * NODES, half), :]
        second = departure[pl.ds(l * NODES + half, half), :]
        return jnp.concatenate([first, second], axis=1)

    def targets(l):
        first = departure[pl.ds(l * NODES, half), :]
        second = departure[pl.ds(l * NODES + half, half), :]
        return jnp.concatenate([first, second], axis=1)

    loads[4].wait()
    slot_ids[...] = lax.broadcasted_iota(jnp.int32, (LANES, 2 * LANES), 0)
    for j in range(sides):
        for c in range(cap):
            at = elements + j * cap + c
            slot_ids[at : at + 1, :] = jnp.full((1, 2 * LANES), jnp.where(c < counts[0, j], at, -1), jnp.int32)

    loads[2].wait()
    for s in range(substeps):
        for l in range(levels):
            state[s, l, slots:, :] = jnp.zeros((LANES - slots, NODES * PADDED), F32)
    for l in range(levels):
        both = targets(l)
        for q in range(half // 2):
            target = jnp.concatenate([both[2 * q : 2 * q + 1, :], both[2 * q + 1 : 2 * q + 2, :]], axis=1)
            pick = jnp.where(slot_ids[...] == target, 1.0, 0.0).astype(BF16)
            picks[l, q, 0:LANES, :] = pick
            picks[l, q, LANES:, :] = pick
    loads[3].wait()
    for s in range(substeps):
        for l in range(levels):
            matrix = weights[s, l]
            mats[s, l] = jnp.transpose(jnp.concatenate([matrix[:, : half * NODES], matrix[:, half * NODES :]], axis=0))

    shift = half * TRACERS % LANES

    def reduce(s, l, c, items):
        value = lowest = highest = None
        for k in range(NODES):
            item = items(k)
            term = mats[s, l, c * NODES + k : c * NODES + k + 1, :] * item
            value = term if k == 0 else value + term
            lowest = item if k == 0 else jnp.minimum(lowest, item)
            highest = item if k == 0 else jnp.maximum(highest, item)
        value = jnp.clip(value, lowest, highest)
        if s + 1 < substeps:
            turned[l, c * PADDED : (c + 1) * PADDED, :] = value
        else:
            turned[l, c * TRACERS : c * TRACERS + PADDED, :] = value
            at = shift + c * TRACERS
            turned_past[l, at : at + PADDED, :] = value

    def receive(s, l):
        rows_of(s, l).wait_recv()

    def arrange(s, l):
        pitch, lanes = (TRACERS, narrow) if s == 0 else (PADDED, NODES * PADDED)
        for j in range(sides):
            at = elements + j * cap
            state[s, l, at : at + cap, 0:lanes] = ends(s)[1][l, j]
        table[l] = jnp.transpose(state[s, l])
        for k in range(NODES):
            block = table[l, k * pitch : k * pitch + PADDED, :]
            high = block.astype(BF16)
            parts[l, k * PADDED : (k + 1) * PADDED, 0:LANES] = high
            parts[l, k * PADDED : (k + 1) * PADDED, LANES:] = (block - high.astype(F32)).astype(BF16)

    def gather(s, l):
        for q in range(half // 2):
            gathered = jnp.dot(parts[l], picks[l, q], preferred_element_type=F32)
            for side in range(2):
                reduce(s, l, 2 * q + side, lambda k: gathered[k * PADDED : (k + 1) * PADDED, side * LANES : (side + 1) * LANES])

    def finish(s, l):
        result = jnp.transpose(turned[l])
        if s + 1 < substeps:
            middle = half * PADDED
            state[s + 1, l, 0:elements, 0:middle] = result[:elements]
            state[s + 1, l, 0:elements, middle:] = result[elements:]
            for j in range(sides):
                for c in range(cap):
                    sent[s, l, j, c : c + 1, :] = state[s + 1, l, pl.ds(asked[j, c, j], 1), :]
        else:
            middle = half * TRACERS
            out[l, :, 0:middle] = result[:elements, :middle]
            out[l, :, middle:narrow] = jnp.transpose(turned_past[l])[elements:, shift : shift + narrow - middle]

    def send(s, l):
        if s + 1 < substeps:
            for step in range(sides):
                row_copy(s + 1, l, jnp.where(upper, step, sides - 1 - step)).start()

    for s in range(substeps):
        receive(s, 0)
        arrange(s, 0)
        for l in range(levels):
            gather(s, l)
            if l + 1 < levels:
                receive(s, l + 1)
                arrange(s, l + 1)
            finish(s, l)
            send(s, l)

    pltpu.make_async_remote_copy(
        src_ref=asked, dst_ref=asked, send_sem=wish_send, recv_sem=wish_got.at[0],
        device_id=device(1), device_id_type=MESH,
    ).wait_send()
    for s in range(substeps):
        source, target = ends(s)
        pltpu.make_async_remote_copy(
            src_ref=source, dst_ref=target, send_sem=row_send.at[s], recv_sem=row_got.at[s, 0],
            device_id=device(1), device_id_type=MESH,
        ).wait_send()


def on_device(tracers, weights, departure, needs, counts):
    substeps, elements, levels, _ = weights.shape
    sides, cap = needs.shape[1:]
    narrow = NODES * TRACERS
    wide = NODES * PADDED
    half = NODES // 2
    far = pl.BlockSpec(memory_space=pl.ANY)
    result = pl.pallas_call(
        kernel,
        out_shape=pltpu.VMEM((levels, elements, narrow), F32),
        in_specs=[far] * 5,
        out_specs=pl.BlockSpec(memory_space=pltpu.VMEM),
        scratch_shapes=[
            pltpu.VMEM((levels, elements, narrow), F32),
            pltpu.VMEM((substeps, levels, elements, NODES * NODES), F32),
            pltpu.VMEM((levels * NODES, elements), jnp.int32),
            pltpu.VMEM((cap, sides), jnp.int32),
            pltpu.SMEM((1, sides), jnp.int32),
            pltpu.SMEM((sides, cap, sides), jnp.int32),
            pltpu.VMEM((LANES, 2 * LANES), jnp.int32),
            pltpu.VMEM((substeps, levels, half * NODES, 2 * elements), F32),
            pltpu.VMEM((substeps, levels, LANES, wide), F32),
            pltpu.VMEM((levels, wide, LANES), F32),
            pltpu.VMEM((levels, half * PADDED, 2 * elements), F32),
            pltpu.VMEM((levels, 3 * LANES, 2 * elements), F32),
            pltpu.VMEM((levels, wide, 2 * LANES), BF16),
            pltpu.VMEM((levels, half // 2, 2 * LANES, 2 * LANES), BF16),
            pltpu.VMEM((levels, sides, cap, narrow), F32),
            pltpu.VMEM((levels, sides, cap, narrow), F32),
            pltpu.VMEM((substeps - 1, levels, sides, cap, wide), F32),
            pltpu.VMEM((substeps - 1, levels, sides, cap, wide), F32),
            pltpu.SemaphoreType.DMA,
            pltpu.SemaphoreType.DMA((sides,)),
            pltpu.SemaphoreType.DMA((substeps,)),
            pltpu.SemaphoreType.DMA((substeps, levels)),
            pltpu.SemaphoreType.DMA((5,)),
        ],
        compiler_params=pltpu.CompilerParams(collective_id=0, has_side_effects=True, vmem_limit_bytes=60 << 20),
    )(
        jnp.transpose(tracers, (1, 0, 2)),
        jnp.transpose(weights, (0, 2, 1, 3)),
        jnp.transpose(departure),
        jnp.transpose(needs, (0, 2, 1)),
        counts,
    )
    return jnp.transpose(result, (1, 0, 2))


def solution(mesh):
    return jax.shard_map(
        on_device,
        mesh=mesh,
        in_specs=(
            P("sfc", None, None),
            P(None, "sfc", None, None),
            P("sfc", None),
            P("sfc", None, None),
            P("sfc", None),
        ),
        out_specs=P("sfc", None, None),
        check_vma=False,
    )
```

```python
import jax
import jax.numpy as jnp
from jax import lax
from jax.experimental import pallas as pl
from jax.experimental.pallas import tpu as pltpu
from jax.sharding import PartitionSpec as P

NODES = 16
TRACERS = 30
PADDED = 32
LANES = 128
MESH = pl.DeviceIdType.MESH
F32 = jnp.float32
BF16 = jnp.bfloat16


def kernel(
    tracers_far, weights_far, departure_far, needs_far, counts_far, out,
    tracers, weights, departure, wish, counts, asked, slot_ids, mats, state, table, turned, turned_past, parts, picks,
    sent_first, got_first, sent, got, wish_send, wish_got, row_send, row_got, loaded,
):
    count = lax.axis_size("sfc")
    me = lax.axis_index("sfc")
    substeps, levels, elements, _ = weights.shape
    sides, cap = asked.shape[0], asked.shape[1]
    reach = sides // 2
    narrow = NODES * TRACERS
    remote = sides * cap
    half = NODES // 2
    slots = elements + remote

    def offset_of(j):
        return j - reach + jnp.where(j < reach, 0, 1)

    def device(offset):
        return (lax.rem(me + offset + count, count),)

    loads = [
        pltpu.make_async_copy(far, near, loaded.at[i])
        for i, (far, near) in enumerate((
            (needs_far.at[0], wish), (tracers_far, tracers), (departure_far, departure), (weights_far, weights),
            (counts_far, counts),
        ))
    ]
    loads[0].start()

    barrier = pltpu.get_barrier_semaphore()
    for j in range(sides):
        o = j - reach if j < reach else j - reach + 1
        pl.semaphore_signal(barrier, inc=1, device_id=device(o), device_id_type=MESH)

    for load in loads[1:]:
        load.start()

    def wish_copy(j):
        return pltpu.make_async_remote_copy(
            src_ref=wish, dst_ref=asked.at[j],
            send_sem=wish_send, recv_sem=wish_got.at[j],
            device_id=device(offset_of(j)), device_id_type=MESH,
        )

    def ends(s):
        return (sent_first, got_first) if s == 0 else (sent.at[s - 1], got.at[s - 1])

    def row_copy(s, l, j):
        source, target = ends(s)
        return pltpu.make_async_remote_copy(
            src_ref=source.at[l, j], dst_ref=target.at[l, j], send_sem=row_send.at[s], recv_sem=row_got.at[s, l],
            device_id=device(-offset_of(j)), device_id_type=MESH,
        )

    def rows_of(s, l):
        source, target = ends(s)
        return pltpu.make_async_remote_copy(
            src_ref=source.at[l], dst_ref=target.at[l], send_sem=row_send.at[s], recv_sem=row_got.at[s, l],
            device_id=device(1), device_id_type=MESH,
        )

    loads[0].wait()
    pl.semaphore_wait(barrier, sides)
    upper = me >= count // 2
    across = me - (count - reach)

    def ask(step):
        return jnp.where(step <= across, sides - 1 - across + step, jnp.where(upper, sides - 1 - step, step))

    def answer(step):
        return jnp.where(step <= across, across - step, jnp.where(upper, step, sides - 1 - step))

    for step in range(sides):
        wish_copy(ask(step)).start()

    loads[1].wait()
    for l in range(levels):
        state[0, l, 0:elements, 0:narrow] = tracers[l]

    past_low = count - 1 - me

    def arrival(step):
        low = jnp.where(step <= me, step, jnp.where(step <= reach, step + reach - 1, me + step - reach))
        high = jnp.where(step <= reach - 1 + past_low, sides - 1 - step, step - reach - past_low)
        return jnp.where(me < reach, low, jnp.where(past_low < reach, high, step))

    for step in range(sides):
        j = arrival(step)
        wish_copy(j).wait_recv()
        for l in range(levels):
            for c in range(cap):
                sent_first[l, j, c : c + 1, :] = tracers[l, pl.ds(asked[j, c, j], 1), :]
        for l in range(levels):
            row_copy(0, l, j).start()

    def targets(l):
        first = departure[pl.ds(l * NODES, half), :]
        second = departure[pl.ds(l * NODES + half, half), :]
        return jnp.concatenate([first, second], axis=1)

    def targets(l):
        first = departure[pl.ds(l * NODES, half), :]
        second = departure[pl.ds(l * NODES + half, half), :]
        return jnp.concatenate([first, second], axis=1)

    loads[4].wait()
    slot_ids[...] = lax.broadcasted_iota(jnp.int32, (LANES, 2 * LANES), 0)
    for j in range(sides):
        for c in range(cap):
            at = elements + j * cap + c
            slot_ids[at : at + 1, :] = jnp.full((1, 2 * LANES), jnp.where(c < counts[0, j], at, -1), jnp.int32)

    loads[2].wait()
    for s in range(substeps):
        for l in range(levels):
            state[s, l, slots:, :] = jnp.zeros((LANES - slots, NODES * PADDED), F32)
    for l in range(levels):
        both = targets(l)
        for q in range(half // 2):
            target = jnp.concatenate([both[2 * q : 2 * q + 1, :], both[2 * q + 1 : 2 * q + 2, :]], axis=1)
            pick = jnp.where(slot_ids[...] == target, 1.0, 0.0).astype(BF16)
            picks[l, q, 0:LANES, :] = pick
            picks[l, q, LANES:, :] = pick
    loads[3].wait()
    for s in range(substeps):
        for l in range(levels):
            matrix = weights[s, l]
            mats[s, l] = jnp.transpose(jnp.concatenate([matrix[:, : half * NODES], matrix[:, half * NODES :]], axis=0))

    shift = half * TRACERS % LANES

    def reduce(s, l, c, items):
        value = lowest = highest = None
        for k in range(NODES):
            item = items(k)
            term = mats[s, l, c * NODES + k : c * NODES + k + 1, :] * item
            value = term if k == 0 else value + term
            lowest = item if k == 0 else jnp.minimum(lowest, item)
            highest = item if k == 0 else jnp.maximum(highest, item)
        value = jnp.clip(value, lowest, highest)
        if s + 1 < substeps:
            turned[l, c * PADDED : (c + 1) * PADDED, :] = value
        else:
            turned[l, c * TRACERS : c * TRACERS + PADDED, :] = value
            at = shift + c * TRACERS
            turned_past[l, at : at + PADDED, :] = value

    def receive(s, l):
        rows_of(s, l).wait_recv()

    def arrange(s, l):
        pitch, lanes = (TRACERS, narrow) if s == 0 else (PADDED, NODES * PADDED)
        for j in range(sides):
            at = elements + j * cap
            state[s, l, at : at + cap, 0:lanes] = ends(s)[1][l, j]
        table[l] = jnp.transpose(state[s, l])
        for k in range(NODES):
            block = table[l, k * pitch : k * pitch + PADDED, :]
            high = block.astype(BF16)
            parts[l, k * PADDED : (k + 1) * PADDED, 0:LANES] = high
            parts[l, k * PADDED : (k + 1) * PADDED, LANES:] = (block - high.astype(F32)).astype(BF16)

    def gather(s, l):
        for q in range(half // 2):
            gathered = jnp.dot(parts[l], picks[l, q], preferred_element_type=F32)
            for side in range(2):
                reduce(s, l, 2 * q + side, lambda k: gathered[k * PADDED : (k + 1) * PADDED, side * LANES : (side + 1) * LANES])

    def finish(s, l):
        result = jnp.transpose(turned[l])
        if s + 1 < substeps:
            middle = half * PADDED
            state[s + 1, l, 0:elements, 0:middle] = result[:elements]
            state[s + 1, l, 0:elements, middle:] = result[elements:]
            for j in range(sides):
                for c in range(cap):
                    sent[s, l, j, c : c + 1, :] = state[s + 1, l, pl.ds(asked[j, c, j], 1), :]
        else:
            middle = half * TRACERS
            out[l, :, 0:middle] = result[:elements, :middle]
            out[l, :, middle:narrow] = jnp.transpose(turned_past[l])[elements:, shift : shift + narrow - middle]

    def send(s, l):
        if s + 1 < substeps:
            for step in range(sides):
                row_copy(s + 1, l, answer(step)).start()

    for s in range(substeps):
        for l in range(levels):
            receive(s, l)
            arrange(s, l)
            gather(s, l)
            finish(s, l)
            send(s, l)

    pltpu.make_async_remote_copy(
        src_ref=asked, dst_ref=asked, send_sem=wish_send, recv_sem=wish_got.at[0],
        device_id=device(1), device_id_type=MESH,
    ).wait_send()
    for s in range(substeps):
        source, target = ends(s)
        pltpu.make_async_remote_copy(
            src_ref=source, dst_ref=target, send_sem=row_send.at[s], recv_sem=row_got.at[s, 0],
            device_id=device(1), device_id_type=MESH,
        ).wait_send()


def on_device(tracers, weights, departure, needs, counts):
    substeps, elements, levels, _ = weights.shape
    sides, cap = needs.shape[1:]
    narrow = NODES * TRACERS
    wide = NODES * PADDED
    half = NODES // 2
    far = pl.BlockSpec(memory_space=pl.ANY)
    result = pl.pallas_call(
        kernel,
        out_shape=pltpu.VMEM((levels, elements, narrow), F32),
        in_specs=[far] * 5,
        out_specs=pl.BlockSpec(memory_space=pltpu.VMEM),
        scratch_shapes=[
            pltpu.VMEM((levels, elements, narrow), F32),
            pltpu.VMEM((substeps, levels, elements, NODES * NODES), F32),
            pltpu.VMEM((levels * NODES, elements), jnp.int32),
            pltpu.VMEM((cap, sides), jnp.int32),
            pltpu.SMEM((1, sides), jnp.int32),
            pltpu.SMEM((sides, cap, sides), jnp.int32),
            pltpu.VMEM((LANES, 2 * LANES), jnp.int32),
            pltpu.VMEM((substeps, levels, half * NODES, 2 * elements), F32),
            pltpu.VMEM((substeps, levels, LANES, wide), F32),
            pltpu.VMEM((levels, wide, LANES), F32),
            pltpu.VMEM((levels, half * PADDED, 2 * elements), F32),
            pltpu.VMEM((levels, 3 * LANES, 2 * elements), F32),
            pltpu.VMEM((levels, wide, 2 * LANES), BF16),
            pltpu.VMEM((levels, half // 2, 2 * LANES, 2 * LANES), BF16),
            pltpu.VMEM((levels, sides, cap, narrow), F32),
            pltpu.VMEM((levels, sides, cap, narrow), F32),
            pltpu.VMEM((substeps - 1, levels, sides, cap, wide), F32),
            pltpu.VMEM((substeps - 1, levels, sides, cap, wide), F32),
            pltpu.SemaphoreType.DMA,
            pltpu.SemaphoreType.DMA((sides,)),
            pltpu.SemaphoreType.DMA((substeps,)),
            pltpu.SemaphoreType.DMA((substeps, levels)),
            pltpu.SemaphoreType.DMA((5,)),
        ],
        compiler_params=pltpu.CompilerParams(collective_id=0, has_side_effects=True, vmem_limit_bytes=60 << 20),
    )(
        jnp.transpose(tracers, (1, 0, 2)),
        jnp.transpose(weights, (0, 2, 1, 3)),
        jnp.transpose(departure),
        jnp.transpose(needs, (0, 2, 1)),
        counts,
    )
    return jnp.transpose(result, (1, 0, 2))


def solution(mesh):
    return jax.shard_map(
        on_device,
        mesh=mesh,
        in_specs=(
            P("sfc", None, None),
            P(None, "sfc", None, None),
            P("sfc", None),
            P("sfc", None, None),
            P("sfc", None),
        ),
        out_specs=P("sfc", None, None),
        check_vma=False,
    )
```
